32 devices in a mesh: rep: 8 (over z, x), tp: 4 (over y, core).
Axes of the slice: x: 2, y: 2, z: 4, core: 2. Of those that a mesh axis runs over, the one named last changes fastest.
Arguments:
- tokens: bfloat16 [64, 4096], P(('rep', 'tp')), may hold values from -6 to 6
- conv_state: bfloat16 [3, 64, 8192], P(None, 'rep', 'tp'), may hold values from -6 to 6
- ssm_state: float32 [64, 16, 8192], P('rep', None, 'tp'), may hold values from -6 to 6
- norm_gains: bfloat16 [2, 4096], P(None, ('rep', 'tp')), may hold values from 0.5 to 1.5
- conv_weight: bfloat16 [4, 8192], P(None, ('rep', 'tp')), may hold values from -3 to 3
- conv_skip: bfloat16 [2, 8192], P(None, ('rep', 'tp')), may hold values from -3 to 3
- step_bias: bfloat16 [8192], P(('rep', 'tp')), may hold values from -5 to -1
- decay_log: bfloat16 [16, 8192], P(None, ('rep', 'tp')), may hold values from 0 to 2.796875
- input_proj: bfloat16 [4096, 2, 8192], P(('rep', 'tp')), may hold values from -0.09375 to 0.09375
- select_proj: bfloat16 [8192, 288], P('tp', 'rep'), may hold values from -0.0625 to 0.0625
- step_proj: bfloat16 [256, 8192], P(('rep', 'tp')), may hold values from -0.375 to 0.375
- output_proj: bfloat16 [8192, 4096], P(None, ('rep', 'tp')), may hold values from -0.0625 to 0.0625
- router: bfloat16 [4096, 16], P(('rep', 'tp')), may hold values from -0.09375 to 0.09375
- expert_proj: bfloat16 [4096, 2, 2, 12288], P(('rep', 'tp')), may hold values from -0.09375 to 0.09375
- expert_ids: int32 [64, 2], P(('rep', 'tp')), may hold values from 0 to 15, as said below
Outputs:
- mamba_out: bfloat16 [64, 4096], P(('rep', 'tp'))
- conv_next: bfloat16 [3, 64, 8192], P(None, 'rep', 'tp')
- ssm_next: float32 [64, 16, 8192], P('rep', None, 'tp')
- expert_hidden: bfloat16 [128, 12288], P('rep', 'tp')
The draws below stay inside these ranges and needn't reach their ends.
Inputs may be any that keep to these rules, and one draw needn't show every extreme that they name: `expert_ids`: each row names two different experts. Within each aligned block of 2 rows (the rows of one device) each expert e < 2 is named by at most 2 rows.
All inputs are finite; a program needn't handle non-finite values.
Results may differ from the reference program's by a relative error of at most 0.04.
Values may be sent and summed in bfloat16 or wider, within the bound.
No kernel may reach another device: no remote copies, remote signals or barrier semaphores. Data moves between devices by JAX's collectives and lax.ppermute only.
A program may use at most 192 MiB of HBM per device.

```python
import jax
import jax.numpy as jnp
from jax import lax

D = 4096
INNER = 8192
STEP_RANK = 256
STATE = 16
TAPS = 4
FF = 12288
EXPERTS = 16
EXP_WIN = 2
CAPACITY = 2
TOK_DEV = 2
REQ = 8
TOKENS = 64
SLOTS = 128
N_REP = 8
N_TP = 4


def draw_expert_ids(key, part):
    blocks = TOKENS // TOK_DEV
    per_replica = REQ // TOK_DEV
    subkeys = jax.random.split(jax.random.fold_in(key, 17), 6)
    counts = jax.random.randint(subkeys[0], (blocks, EXP_WIN), 1, CAPACITY + 1)
    full_replica = jax.random.randint(subkeys[1], (), 0, blocks // per_replica)
    replica_of = jnp.arange(blocks, dtype=jnp.int32) // per_replica
    counts = jnp.where((replica_of == full_replica)[:, None], CAPACITY, counts)
    scores = jax.random.randint(subkeys[2], (blocks, TOK_DEV, EXP_WIN), 0, 1 << 20) * TOK_DEV + jnp.arange(TOK_DEV, dtype=jnp.int32)[None, :, None]
    ordering = jnp.argsort(scores, axis=1)
    order_rank = jnp.argsort(ordering, axis=1)
    member = order_rank < counts[:, None, :]
    in_first = member[:, :, 0]
    in_second = member[:, :, 1]
    spare = EXPERTS - EXP_WIN
    spare_one = EXP_WIN + jax.random.randint(subkeys[3], (blocks, TOK_DEV), 0, spare)
    spare_two = EXP_WIN + (spare_one - EXP_WIN + jax.random.randint(subkeys[4], (blocks, TOK_DEV), 1, spare)) % spare
    first_pick = jnp.where(in_first, 0, jnp.where(in_second, 1, spare_one))
    second_pick = jnp.where(in_first & in_second, 1, jnp.where(in_first | in_second, spare_one, spare_two))
    swapped = jax.random.randint(subkeys[5], (blocks, TOK_DEV), 0, 2) == 1
    column_one = jnp.where(swapped, second_pick, first_pick)
    column_two = jnp.where(swapped, first_pick, second_pick)
    return jnp.stack([column_one, column_two], axis=-1).reshape(TOKENS, 2).astype(jnp.int32)


def shard_levels(key, extent, cuts, least, top_value):
    def one(axis_at, blocks):
        draws = jax.random.uniform(jax.random.fold_in(jax.random.fold_in(key, 6), axis_at), (blocks,), jnp.float32, least / len(cuts), top_value / len(cuts))
        return jnp.repeat(jnp.exp(draws), extent[axis_at] // blocks).reshape((-1,) + (1,) * (len(extent) - axis_at - 1))

    level = one(*cuts[0])
    for cut in cuts[1:]:
        level = level * one(*cut)
    return level


def normal_values(own_key, dims, scale, bound, cuts=(), held_as=jnp.bfloat16):
    level = shard_levels(own_key, dims, cuts, -0.22, 0.18) if cuts else 1.0
    array = jax.random.normal(own_key, dims, jnp.float32) * scale * level
    return jnp.minimum(jnp.maximum(array, -bound), bound).astype(held_as)


def setup_inputs(seed: int = 0) -> dict:
    splits = jax.random.split(jax.random.key(seed), 16)
    return {
        "tokens": normal_values(splits[0], (TOKENS, D), 1.0, 6.0, ((0, 32),)),
        "conv_state": normal_values(splits[1], (TAPS - 1, TOKENS, INNER), 1.0, 6.0, ((1, 8), (2, 4))),
        "ssm_state": normal_values(splits[2], (TOKENS, STATE, INNER), 1.0, 6.0, ((0, 8), (2, 4)), jnp.float32),
        "norm_gains": jnp.clip(1.0 + 0.1 * jax.random.normal(splits[3], (2, D), jnp.float32), 0.5, 1.5).astype(jnp.bfloat16),
        "conv_weight": normal_values(splits[4], (TAPS, INNER), 0.5, 3.0, ((1, 32),)),
        "conv_skip": normal_values(splits[5], (2, INNER), 0.5, 3.0, ((1, 32),)),
        "step_bias": jnp.clip(-5.0 + 4.0 * jax.random.uniform(splits[6], (INNER,), jnp.float32) ** shard_levels(splits[6], (INNER,), ((0, 32),), -0.2, 0.2), -5.0, -1.0).astype(jnp.bfloat16),
        "decay_log": jnp.clip(2.796875 * jax.random.uniform(splits[7], (STATE, INNER), jnp.float32) ** shard_levels(splits[7], (STATE, INNER), ((1, 32),), -0.2, 0.2), 0.0, 2.796875).astype(jnp.bfloat16),
        "input_proj": normal_values(splits[8], (D, 2, INNER), D ** -0.5, 0.09375, ((0, 32),)),
        "select_proj": normal_values(splits[9], (INNER, STEP_RANK + 2 * STATE), INNER ** -0.5, 0.0625, ((0, 4), (1, 8))),
        "step_proj": normal_values(splits[10], (STEP_RANK, INNER), STEP_RANK ** -0.5, 0.375, ((0, 32),)),
        "output_proj": normal_values(splits[11], (INNER, D), INNER ** -0.5, 0.0625, ((1, 32),)),
        "router": normal_values(splits[12], (D, EXPERTS), D ** -0.5, 0.09375, ((0, 32),)),
        "expert_proj": normal_values(splits[13], (D, EXP_WIN, 2, FF), D ** -0.5, 0.09375, ((0, 32),)),
        "expert_ids": draw_expert_ids(jax.random.fold_in(splits[15], 71), 0),
    }


epsilon = 1e-05

def norm_scale(values, gain):
    mean_square = lax.optimization_barrier(jnp.mean(values * values, axis=-1, keepdims=True))
    return values * lax.rsqrt(mean_square + epsilon) * gain.astype(jnp.float32)

def ssm_block(block_args):
    state, step_size, activated, input_map, output_map, decay_rate = block_args
    factor = jnp.exp(step_size[:, None, :] * decay_rate[None])
    state_next = factor * state + (step_size * activated)[:, None, :] * input_map[:, :, None]
    readout = lax.optimization_barrier(jnp.sum(state_next * output_map[:, :, None], axis=1))
    return (state_next, readout)

def reference(tokens, conv_state, ssm_state, norm_gains, conv_weight, conv_skip, step_bias, decay_log, input_proj, select_proj, step_proj, output_proj, router, expert_proj, expert_ids):
    residual_in = tokens.astype(jnp.float32)
    normed = norm_scale(residual_in, norm_gains[0]).astype(jnp.bfloat16)
    projected = jnp.dot(normed, input_proj.reshape(D, 2 * INNER), preferred_element_type=jnp.float32)
    conv_input = projected[:, :INNER]
    gate_z = projected[:, INNER:]
    conv_taps = conv_weight.astype(jnp.float32)
    history = conv_state.astype(jnp.float32)
    conv_mix = lax.optimization_barrier(jnp.sum(conv_taps[:-1, None, :] * history, axis=0)) + conv_taps[-1] * conv_input + conv_skip[0].astype(jnp.float32)
    conv_next = jnp.concatenate([conv_state[1:], conv_input.astype(jnp.bfloat16)[None]], axis=0)
    activated = jax.nn.silu(conv_mix)
    selected = jnp.dot(activated.astype(jnp.bfloat16), select_proj, preferred_element_type=jnp.float32)
    step_low = selected[:, :STEP_RANK].astype(jnp.bfloat16)
    input_map = selected[:, STEP_RANK:STEP_RANK + STATE]
    output_map = selected[:, STEP_RANK + STATE:]
    step_size = jax.nn.softplus(jnp.dot(step_low, step_proj, preferred_element_type=jnp.float32) + step_bias.astype(jnp.float32))
    decay_rate = -jnp.exp(decay_log.astype(jnp.float32))
    replicas = TOKENS // REQ
    state_next, readout = lax.map(lambda block_args: ssm_block(block_args + (decay_rate,)), (ssm_state.reshape(replicas, REQ, STATE, INNER), step_size.reshape(replicas, REQ, INNER), activated.reshape(replicas, REQ, INNER), input_map.reshape(replicas, REQ, STATE), output_map.reshape(replicas, REQ, STATE)))
    ssm_next = state_next.reshape(TOKENS, STATE, INNER)
    readout = readout.reshape(TOKENS, INNER) + conv_skip[1].astype(jnp.float32) * activated
    gated_out = (readout * jax.nn.silu(gate_z)).astype(jnp.bfloat16)
    inner_block = INNER // N_TP
    mixer_out = jnp.zeros((TOKENS, D), jnp.float32)
    for block_index in range(N_TP):
        lower = block_index * inner_block
        partial_out = jnp.dot(gated_out[:, lower:lower + inner_block], output_proj[lower:lower + inner_block], preferred_element_type=jnp.float32)
        mixer_out = mixer_out + lax.optimization_barrier(partial_out.astype(jnp.bfloat16)).astype(jnp.float32)
    residual = residual_in + mixer_out
    mamba_out = residual.astype(jnp.bfloat16)
    moe_in = norm_scale(residual, norm_gains[1]).astype(jnp.bfloat16)
    logits = jnp.dot(moe_in, router, preferred_element_type=jnp.float32)
    choose = (expert_ids[:, :, None] == jnp.arange(EXPERTS, dtype=jnp.int32)[None, None, :]).astype(jnp.float32)
    picked = lax.optimization_barrier(jnp.sum(choose * logits[:, None, :], axis=2))
    first_gate = jax.nn.sigmoid(picked[:, 0] - picked[:, 1])
    second_gate = jax.nn.sigmoid(picked[:, 1] - picked[:, 0])
    window = jnp.arange(EXP_WIN, dtype=jnp.int32)
    names_first = expert_ids[:, 0:1] == window[None, :]
    names_second = expert_ids[:, 1:2] == window[None, :]
    zero = jnp.zeros((), jnp.float32)
    gate_w = jnp.where(names_first, first_gate[:, None], zero) + jnp.where(names_second, second_gate[:, None], zero)
    routed = (names_first | names_second).astype(jnp.int32)
    blocks = TOKENS // TOK_DEV
    routed_blocks = routed.reshape(blocks, TOK_DEV, EXP_WIN)
    position = jnp.cumsum(routed_blocks, axis=1) - routed_blocks
    slot_of = ((position[..., None] == jnp.arange(CAPACITY, dtype=jnp.int32)) & (routed_blocks[..., None] > 0)).astype(jnp.float32)
    slot_x = jnp.einsum('btec,btd->becd', slot_of, moe_in.reshape(blocks, TOK_DEV, D).astype(jnp.float32)).astype(jnp.bfloat16)
    slot_gate = jnp.einsum('btec,bte->bec', slot_of, gate_w.reshape(blocks, TOK_DEV, EXP_WIN)).astype(jnp.bfloat16)
    feature_block = D // N_REP
    hidden_list = []
    for expert in range(EXP_WIN):
        slot_rows = slot_x[:, expert].reshape(blocks * CAPACITY, D)
        gate_up = jnp.zeros((blocks * CAPACITY, 2 * FF), jnp.float32)
        for block_index in range(N_REP):
            lower = block_index * feature_block
            partial_up = jnp.dot(slot_rows[:, lower:lower + feature_block], expert_proj[lower:lower + feature_block, expert].reshape(feature_block, 2 * FF), preferred_element_type=jnp.float32)
            gate_up = gate_up + lax.optimization_barrier(partial_up.astype(jnp.bfloat16)).astype(jnp.float32)
        slot_scale = slot_gate[:, expert].reshape(blocks * CAPACITY).astype(jnp.float32)
        hidden = slot_scale[:, None] * jax.nn.silu(gate_up[:, :FF]) * gate_up[:, FF:]
        hidden_list.append(hidden.reshape(blocks, CAPACITY, FF))
    expert_hidden = jnp.stack(hidden_list, axis=1).reshape(SLOTS, FF).astype(jnp.bfloat16)
    return (mamba_out, conv_next, ssm_next, expert_hidden)
```

```python
import jax
import jax.numpy as jnp
from jax import lax
from jax.experimental import pallas as pl
from jax.experimental.pallas import tpu as pltpu
from jax.sharding import PartitionSpec as P

CAPACITY = 2
LANES = 128
INTERPRET = False
AXES = ("rep", "tp")
epsilon = 1e-05
bf16 = jnp.bfloat16
f32 = jnp.float32


def swap(value, mask):
    count = lax.axis_size(AXES)
    return lax.ppermute(value, AXES, [(i, i ^ mask) for i in range(count)])


def mask_of(index, masks):
    total = 0
    for k, mask in enumerate(reversed(masks)):
        total = total + ((index >> k) & 1) * mask
    return total


def gather_bits(value, groups):
    for group in groups:
        parts = []
        for combo in range(1 << len(group)):
            mask = sum(m for k, m in enumerate(group) if (combo >> k) & 1)
            parts.append(swap(value, mask) if mask else value)
        value = jnp.stack(parts).reshape((2,) * len(group) + value.shape)
    return value


def take_bit(value, axis, which):
    return lax.index_in_dim(value, which, axis, keepdims=False)


def add_bf(left, right):
    return (left.astype(f32) + right.astype(f32)).astype(bf16)


def scatter_bits(values, names, orders):
    names = [list(names) for _ in values]
    for step in range(len(orders[0])):
        received = []
        for k, value in enumerate(values):
            axis = names[k].index(orders[k][step])
            received.append(swap(take_bit(value, axis, 1), orders[k][step]))
        for k, value in enumerate(values):
            axis = names[k].index(orders[k][step])
            values[k] = add_bf(take_bit(value, axis, 0), received[k])
            names[k].pop(axis)
    return values


def color_widths(width):
    blocks = width // LANES
    if blocks < 3 or width % LANES:
        return [width]
    base = blocks // 3
    extra = blocks - 3 * base
    return [(base + (k < extra)) * LANES for k in range(3)]


def spread_rows(rows):
    count, depth = rows.shape
    eye = jnp.eye(2, dtype=rows.dtype)
    wide = eye[:, None, None, :] * rows[None, :, :, None]
    return wide.reshape(2 * count, 2 * depth)


def pair_kernel(widths):
    def body(index_ref, rows_ref, weight_ref, *out_refs):
        weight = weight_ref[...]
        depth = weight.shape[0] * weight.shape[1]
        result = jnp.dot(
            rows_ref[...], weight.reshape(depth, weight.shape[2]), preferred_element_type=f32
        ).astype(bf16)
        start = 0
        for out_ref, width in zip(out_refs, widths):
            out_ref[...] = result[:, start : start + width].reshape(out_ref.shape)
            start += width

    return body


def pair_matmul(rows, weight, tp_index, tp_masks, fixed, width, widths):
    depth, experts = weight.shape[0], weight.shape[1]
    count = rows.shape[0] // 2
    blocks = 1 << len(tp_masks)
    grid_spec = pltpu.PrefetchScalarGridSpec(
        num_scalar_prefetch=1,
        grid=(blocks, experts),
        in_specs=[
            pl.BlockSpec(rows.shape, lambda g, e, s: (0, 0)),
            pl.BlockSpec(
                (depth, None, 2, width),
                lambda g, e, s: (0, e, 0, s[0] ^ (fixed + mask_of(g, tp_masks))),
            ),
        ],
        out_specs=[
            pl.BlockSpec((None, None, 2, count, w), lambda g, e, s: (g, e, 0, 0, 0))
            for w in widths
        ],
    )
    return pl.pallas_call(
        pair_kernel(widths),
        grid_spec=grid_spec,
        out_shape=[jax.ShapeDtypeStruct((blocks, experts, 2, count, w), bf16) for w in widths],
        interpret=INTERPRET,
        name="pair_matmul",
    )(tp_index.reshape(1), rows, weight)


def out_kernel(index_ref, start_ref, gated_ref, weight_ref, out_ref):
    @pl.when(pl.program_id(0) == 0)
    def _():
        out_ref[...] = start_ref[...].astype(f32)

    out_ref[...] += jnp.dot(gated_ref[...], weight_ref[...], preferred_element_type=f32)


def out_matmul(start, gated, weight, tp_index, tp_masks):
    blocks, rows, width = gated.shape
    columns = weight.shape[1]
    grid_spec = pltpu.PrefetchScalarGridSpec(
        num_scalar_prefetch=1,
        grid=(blocks,),
        in_specs=[
            pl.BlockSpec(start.shape, lambda g, s: (0, 0)),
            pl.BlockSpec((None, rows, width), lambda g, s: (g, 0, 0)),
            pl.BlockSpec((width, columns), lambda g, s: (s[0] ^ mask_of(g, tp_masks), 0)),
        ],
        out_specs=pl.BlockSpec((rows, columns), lambda g, s: (0, 0)),
    )
    return pl.pallas_call(
        out_kernel,
        grid_spec=grid_spec,
        out_shape=jax.ShapeDtypeStruct((rows, columns), f32),
        interpret=INTERPRET,
        name="out_matmul",
    )(tp_index.reshape(1), start, gated, weight)


def split_scatter(rows, weight, tp_index, core_mask, tp_masks, rep_masks, orders_of):
    width = weight.shape[3] // (2 << len(tp_masks))
    widths = color_widths(width)
    count = rows.shape[0] // 2
    experts = weight.shape[1]
    reps = 1 << len(rep_masks)
    per_rep = count // reps
    args = (rows, weight, tp_index, tp_masks)
    send = pair_matmul(*args, core_mask, width, widths)
    got = [swap(part, core_mask) for part in send]
    rows_two = lax.optimization_barrier((rows, send))[0]
    keep = pair_matmul(rows_two, *args[1:], 0, width, widths)
    parts = []
    for mine, other in zip(keep, got):
        total = add_bf(mine, other)
        parts.append(
            total.reshape(
                (2,) * len(tp_masks)
                + (experts, 2)
                + (2,) * len(rep_masks)
                + (per_rep, total.shape[-1])
            )
        )
    names = list(tp_masks) + [None, None] + list(rep_masks)
    parts = scatter_bits(parts, names, [orders_of(k) for k in range(len(parts))])
    return jnp.concatenate(parts, axis=-1)


def shards(
    tokens,
    conv_state,
    ssm_state,
    norm_gains,
    conv_weight,
    conv_skip,
    step_bias,
    decay_log,
    input_proj,
    select_proj,
    step_proj,
    output_proj,
    router,
    expert_proj,
    expert_ids,
):
    tp_count = lax.axis_size("tp")
    rep_count = lax.axis_size("rep")
    devices = tp_count * rep_count
    tp_index = lax.axis_index("tp").astype(jnp.int32)
    rep_index = lax.axis_index("rep").astype(jnp.int32)
    tp_bits = [1 << k for k in range(tp_count.bit_length() - 1)]
    rep_bits = [1 << k for k in range(rep_count.bit_length() - 1)]
    core_mask = tp_bits[0]
    rep_order = [rep_bits[-1 - k] for k in range(len(rep_bits))]
    far = [m * tp_count for m in rep_order]
    rows_masks = list(reversed(rep_order))
    rows_joint = [m * tp_count for m in rows_masks]
    tp_rest = tp_bits[1:]
    near = [far[-1]] + tp_rest
    groups = [far[:-1][k : k + 2] for k in range(0, len(far) - 1, 2)]
    groups += [near[k : k + 2] for k in range(0, len(near), 2)] + [[core_mask]]
    tp_outer = [core_mask] + list(reversed(tp_rest))

    base_order = list(reversed(tp_rest)) + list(reversed(far))

    def orders_of(k):
        head, tail = base_order[:3], base_order[3:]
        return head[k % 3 :] + head[: k % 3] + tail

    tok_dev, model = tokens.shape
    feature_dev = model // devices
    inner_dev = ssm_state.shape[2]
    state_count = ssm_state.shape[1]
    per_rep = tok_dev * tp_count
    total_tokens = tok_dev * devices

    residual_in = tokens.astype(f32)
    scale = lax.rsqrt(jnp.mean(residual_in * residual_in, axis=-1, keepdims=True) + epsilon)
    unit = (residual_in * scale).astype(bf16)
    both = jnp.stack([tokens, unit]).reshape(2, tok_dev, devices, feature_dev)
    both = both.transpose(2, 0, 1, 3).reshape(devices, 2 * tok_dev, feature_dev)

    params = jnp.concatenate([conv_weight, conv_skip, step_bias[None], decay_log], axis=0)
    block_of = [(b // tp_count, b % tp_count) for b in range(devices)]
    homes = [
        (b, (b % rep_count) * tp_count + b // rep_count) for b in range(devices)
    ]
    params = lax.ppermute(params, AXES, homes)
    rep_groups = [[m] for m in far]
    params_rel = gather_bits(params, rep_groups)
    params_rel = params_rel.reshape((rep_count,) + params.shape)
    select_rel = gather_bits(select_proj.T, rep_groups)
    select_rel = select_rel.reshape(rep_count, select_proj.shape[1], inner_dev)
    step_rows = step_proj.shape[0]
    step_parts = [
        swap_slice(step_proj, tp_index, d, inner_dev) for d in range(tp_count)
    ]
    step_rel = gather_bits(jnp.stack(step_parts), rep_groups)
    step_rel = step_rel.reshape(devices * step_rows, inner_dev)
    ids_parts = [expert_ids if d == 0 else swap(expert_ids, d) for d in range(tp_count)]
    ids_rel = jnp.stack(ids_parts)
    ids_all = jnp.stack(
        [lax.dynamic_index_in_dim(ids_rel, t ^ tp_index, 0, keepdims=False) for t in range(tp_count)]
    ).reshape(per_rep, 2)

    row_block = jnp.arange(total_tokens, dtype=jnp.int32)
    absolute_row = (rep_index ^ mask_of(row_block // per_rep, rows_masks)) * per_rep + (
        row_block % per_rep
    )
    to_rel = (absolute_row[:, None] == row_block[None, :]).astype(bf16)

    spread = lax.all_to_all(both, AXES, split_axis=0, concat_axis=0, tiled=True)
    spread = spread.reshape(devices, 2, tok_dev, feature_dev).transpose(0, 2, 1, 3)
    spread = spread.reshape(total_tokens, 2 * feature_dev)
    spread = jnp.dot(to_rel, spread, preferred_element_type=f32)
    block_in = spread[:, :feature_dev]
    gains = norm_gains.astype(f32)
    rows_in = (spread[:, feature_dev:] * gains[0]).astype(bf16)

    projected = split_scatter(
        spread_rows(rows_in),
        input_proj[:, None],
        tp_index,
        core_mask,
        list(reversed(tp_rest)),
        rows_joint,
        orders_of,
    )[0].astype(f32)
    conv_input = projected[0]
    gate_z = projected[1]

    params_all = jnp.concatenate(
        [
            lax.dynamic_index_in_dim(
                params_rel, rel_index(r ^ rep_index, rows_masks), 0, keepdims=False
            )
            for r in range(rep_count)
        ],
        axis=-1,
    ).astype(f32)
    taps = conv_weight.shape[0]
    conv_taps = params_all[:taps]
    skip_rows = params_all[taps : taps + 2]
    shift_dev = params_all[taps + 2]
    decay_dev = params_all[taps + 3 :]

    history = conv_state.astype(f32)
    conv_mix = (
        jnp.sum(conv_taps[:-1, None, :] * history, axis=0)
        + conv_taps[-1] * conv_input
        + skip_rows[0]
    )
    conv_next = jnp.concatenate([conv_state[1:], conv_input.astype(bf16)[None]], axis=0)
    activated = jax.nn.silu(conv_mix)
    select_cols = select_rel.shape[0] * select_rel.shape[1]
    select_part = lax.dot_general(
        activated.astype(bf16),
        select_rel.reshape(select_cols, inner_dev),
        (((1,), (1,)), ((), ())),
        preferred_element_type=f32,
    )
    selected = select_part
    for d in range(1, tp_count):
        selected = selected + swap(select_part, d)
    selected = selected.astype(bf16)
    step_rank = devices * step_rows
    column = jnp.arange(select_cols, dtype=jnp.int32)
    per_block = select_proj.shape[1]
    absolute_col = (rep_index ^ mask_of(column // per_block, rows_masks)) * per_block + (
        column % per_block
    )
    rank = jnp.arange(step_rank, dtype=jnp.int32)
    rank_dev = rank // step_rows
    rank_rep = rep_index ^ mask_of(rank_dev // tp_count, rows_masks)
    rank_tp = tp_index ^ (rank_dev % tp_count)
    wanted = (rank_rep * tp_count + rank_tp) * step_rows + rank % step_rows
    wanted = jnp.concatenate([wanted, jnp.arange(step_rank, select_cols, dtype=jnp.int32)])
    reorder = (absolute_col[:, None] == wanted[None, :]).astype(bf16)
    selected = jnp.dot(selected, reorder, preferred_element_type=f32)
    step_low = selected[:, :step_rank].astype(bf16)
    input_map = selected[:, step_rank : step_rank + state_count]
    output_map = selected[:, step_rank + state_count :]
    step_size = jax.nn.softplus(
        jnp.dot(step_low, step_rel, preferred_element_type=f32) + shift_dev
    )
    decay_rate = -jnp.exp(decay_dev)
    factor = jnp.exp(step_size[:, None, :] * decay_rate[None])
    ssm_next = factor * ssm_state + (step_size * activated)[:, None, :] * input_map[:, :, None]
    readout = jnp.sum(ssm_next * output_map[:, :, None], axis=1) + skip_rows[1] * activated
    gated_out = (readout * jax.nn.silu(gate_z)).astype(bf16)

    gated_all = gather_bits(gated_out, groups).reshape(tp_count, total_tokens, inner_dev)
    residual = out_matmul(block_in, gated_all, output_proj, tp_index, tp_outer)
    rows_moe = (residual * gains[1]).astype(bf16)

    summed = split_scatter(
        spread_rows(rows_moe),
        expert_proj,
        tp_index,
        core_mask,
        list(reversed(tp_rest)),
        rows_joint,
        orders_of,
    ).astype(f32)

    expert_total = router.shape[1]
    partial = jnp.concatenate(
        [
            jnp.dot(rows_moe, router, preferred_element_type=f32),
            jnp.sum(residual * residual, axis=-1, keepdims=True),
        ],
        axis=-1,
    )
    high = lax.reduce_precision(partial, 8, 7)
    low = partial - high
    half = LANES // 2
    facts = jnp.concatenate([high, low], axis=-1).astype(bf16)
    facts = jnp.pad(facts, ((0, 0), (0, half - facts.shape[1])))
    outgoing = jnp.concatenate([residual.astype(bf16), facts], axis=-1)
    outgoing = lax.dot_general(
        to_rel, outgoing, (((0,), (0,)), ((), ())), preferred_element_type=f32
    ).astype(bf16)
    out_rows = outgoing[:, :feature_dev].reshape(devices, tok_dev * feature_dev)
    out_facts = outgoing[:, feature_dev:].reshape(rep_count, 1, per_rep * half)
    out_facts = jnp.broadcast_to(out_facts, (rep_count, tp_count, per_rep * half))
    out_facts = out_facts.reshape(devices, per_rep * half)
    outgoing = jnp.concatenate([out_rows, out_facts], axis=-1)
    incoming = lax.all_to_all(outgoing, AXES, split_axis=0, concat_axis=0, tiled=True)
    mamba_out = incoming[:, : tok_dev * feature_dev].reshape(devices, tok_dev, feature_dev)
    mamba_out = mamba_out.transpose(1, 0, 2).reshape(tok_dev, model)
    facts = incoming[:, tok_dev * feature_dev :].astype(f32).sum(axis=0).reshape(per_rep, half)
    facts = facts[:, : expert_total + 1] + facts[:, expert_total + 1 : 2 * (expert_total + 1)]
    moe_scale = lax.rsqrt(facts[:, expert_total:] / model + epsilon)
    logits = facts[:, :expert_total] * moe_scale

    choose = (
        ids_all[:, :, None] == jnp.arange(expert_total, dtype=jnp.int32)[None, None, :]
    ).astype(f32)
    picked = jnp.sum(choose * logits[:, None, :], axis=2)
    first_gate = jax.nn.sigmoid(picked[:, 0] - picked[:, 1])
    second_gate = jax.nn.sigmoid(picked[:, 1] - picked[:, 0])
    window_count = expert_proj.shape[1]
    window = jnp.arange(window_count, dtype=jnp.int32)
    names_first = ids_all[:, 0:1] == window[None, :]
    names_second = ids_all[:, 1:2] == window[None, :]
    zero = jnp.zeros((), f32)
    gate_w = jnp.where(names_first, first_gate[:, None], zero) + jnp.where(
        names_second, second_gate[:, None], zero
    )
    gate_w = gate_w.astype(bf16).astype(f32)
    routed = (names_first | names_second).astype(jnp.int32).reshape(tp_count, tok_dev, window_count)
    position = jnp.cumsum(routed, axis=1) - routed
    slot_of = (position[..., None] == jnp.arange(CAPACITY, dtype=jnp.int32)) & (
        routed[..., None] > 0
    )
    gate_up = summed * moe_scale[None, None]
    hidden = gate_w.T[:, :, None] * jax.nn.silu(gate_up[:, 0]) * gate_up[:, 1]
    hidden = hidden.astype(bf16).reshape(window_count, tp_count, tok_dev, -1)
    expert_hidden = jnp.einsum(
        "jtec,ejtf->jecf", slot_of.astype(bf16), hidden, preferred_element_type=f32
    ).astype(bf16)
    expert_hidden = expert_hidden.reshape(tp_count * window_count * CAPACITY, -1)
    return (mamba_out, conv_next, ssm_next, expert_hidden)


def rel_index(mask, masks):
    total = 0
    for k, m in enumerate(reversed(masks)):
        total = total + jnp.where((mask & m) != 0, 1 << k, 0)
    return total


def swap_slice(value, tp_index, d, width):
    piece = lax.dynamic_slice_in_dim(value, (tp_index ^ d) * width, width, 1)
    return swap(piece, d) if d else piece


def solution(mesh):
    in_specs = (
        P(("rep", "tp"), None),
        P(None, "rep", "tp"),
        P("rep", None, "tp"),
        P(None, ("rep", "tp")),
        P(None, ("rep", "tp")),
        P(None, ("rep", "tp")),
        P(("rep", "tp")),
        P(None, ("rep", "tp")),
        P(("rep", "tp"), None, None),
        P("tp", "rep"),
        P(("rep", "tp"), None),
        P(None, ("rep", "tp")),
        P(("rep", "tp"), None),
        P(("rep", "tp"), None, None, None),
        P(("rep", "tp"), None),
    )
    out_specs = (P(("rep", "tp"), None), P(None, "rep", "tp"), P("rep", None, "tp"), P("rep", "tp"))
    return jax.shard_map(shards, mesh=mesh, in_specs=in_specs, out_specs=out_specs, check_vma=False)
```

```python
import jax
import jax.numpy as jnp
from jax import lax
from jax.experimental import pallas as pl
from jax.experimental.pallas import tpu as pltpu
from jax.sharding import PartitionSpec as P

CAPACITY = 2
LANES = 128
INTERPRET = False
AXES = ("rep", "tp")
epsilon = 1e-05
bf16 = jnp.bfloat16
f32 = jnp.float32


def swap(value, mask):
    count = lax.axis_size(AXES)
    return lax.ppermute(value, AXES, [(i, i ^ mask) for i in range(count)])


def mask_of(index, masks):
    total = 0
    for k, mask in enumerate(reversed(masks)):
        total = total ^ (((index >> k) & 1) * mask)
    return total


def index_of(mask, masks):
    count = 1 << len(masks)
    table = {mask_of(i, masks): i for i in range(count)}
    if isinstance(mask, int):
        return table[mask]
    total = 0
    for k in range(len(masks)):
        total = total ^ (((mask >> k) & 1) * table[1 << k])
    return total


def after(value, *others):
    return lax.optimization_barrier((value, others))[0]


def gather_stage(value, group):
    parts = []
    for combo in range(1 << len(group)):
        mask = mask_of(combo, list(reversed(group)))
        parts.append(swap(value, mask) if mask else value)
    return jnp.stack(parts).reshape((-1,) + value.shape[1:])


def take_bit(value, axis, which):
    return lax.index_in_dim(value, which, axis, keepdims=False)


def add_bf(left, right):
    return (left.astype(f32) + right.astype(f32)).astype(bf16)


def scatter_bits(chains, hook, merge=False):
    chains = [list(chain) for chain in chains]
    for step in range(len(chains[0][3])):
        sends = []
        gots = []
        for chain in chains:
            keep, send, names, order = chain
            if step:
                axis = names.index(order[step])
                left, right = keep
                send = add_bf(take_bit(left, axis, 1), take_bit(right, axis, 1))
                keep = add_bf(take_bit(left, axis, 0), take_bit(right, axis, 0))
                chain[2] = names[:axis] + names[axis + 1 :]
            sends.append(send.reshape((-1,) + send.shape[-2:]))
            chain[0] = keep
        if merge and step == len(chains[0][3]) - 1:
            chains[0][0] = jnp.concatenate([chain[0] for chain in chains], axis=-1)
            chains = chains[:1]
            sends = [jnp.concatenate(sends, axis=-1)]
        for chain, flat in zip(chains, sends):
            gots.append(swap(flat, chain[3][step]).reshape(chain[0].shape))
        gots = hook(step, sends, gots)
        for chain, got in zip(chains, gots):
            chain[0] = (chain[0], got)
    return [left.astype(f32) + right.astype(f32) for (left, right), *_ in chains]


def color_widths(width):
    blocks = width // LANES
    if blocks < 3 or width % LANES:
        return [width]
    base = blocks // 3
    extra = blocks - 3 * base
    return [(base + (k < extra)) * LANES for k in range(3)]


def split_at(rows, position):
    half = rows >> (position + 1)
    return [
        [(o * 2 * half + bit * half, half) for o in range(1 << position)] for bit in range(2)
    ]


def pair_matmul(rows, weight, tp_index, tp_masks, fixed, half, pieces, addend=None, into=None):
    source, pick, gain = rows
    depth, experts = weight.shape[0], weight.shape[1]
    count = source.shape[0] if pick is None else pick.shape[0]
    blocks = 1 << (len(tp_masks) - 1)
    width = weight.shape[3] // (4 * blocks)
    outer = fixed ^ (tp_masks[0] if half else 0)
    small = [source] + ([] if pick is None else [pick]) + [gain]
    into = [] if into is None else into

    def body(index_ref, *refs):
        refs = list(refs)
        rows_ref = refs.pop()
        source_ref = refs.pop(0)
        pick_ref = None if pick is None else refs.pop(0)
        gain_ref = refs.pop(0)
        weight_ref = refs.pop(0)
        addend_ref = None if addend is None else refs.pop(0)
        out_refs = refs[len(into) :]

        @pl.when((pl.program_id(0) == 0) & (pl.program_id(1) == 0))
        def _():
            picked = source_ref[...]
            if pick_ref is not None:
                picked = jnp.dot(pick_ref[...], picked, preferred_element_type=f32)
            scaled = (picked * gain_ref[...]).astype(bf16)
            row = lax.broadcasted_iota(jnp.int32, (depth, 2 * depth), 0)
            column = lax.broadcasted_iota(jnp.int32, (depth, 2 * depth), 1)
            for x in range(2):
                place = jnp.where(column == 2 * row + x, 1.0, 0.0).astype(bf16)
                wide = jnp.dot(scaled, place, preferred_element_type=f32)
                rows_ref[x * count : (x + 1) * count, :] = wide.astype(bf16)

        result = jnp.dot(
            rows_ref[...],
            weight_ref[...].reshape(2 * depth, width),
            preferred_element_type=f32,
        )
        if addend_ref is not None:
            result = result + addend_ref[...].reshape(2 * count, width).astype(f32)
        result = result.astype(bf16)
        targets = iter(out_refs)
        for planes, first, columns, split in pieces:
            groups = [[(0, count)]] if split is None else split_at(count, split)
            for group in groups:
                target = next(targets)
                for k, plane in enumerate(planes):
                    base = 0
                    for start, size in group:
                        low = plane * count + start
                        target[k, base : base + size, :] = result[
                            low : low + size, first : first + columns
                        ]
                        base += size

    out_specs, out_shape = [], []
    for planes, _, columns, split in pieces:
        number = len(planes)
        if split is None:
            outs, lead, shift, size = 1, blocks, 0, count
        else:
            outs, lead, shift, size = 2, 2 * blocks, half * blocks, count // 2
        for _ in range(outs):
            out_specs.append(
                pl.BlockSpec(
                    (None, None, number, size, columns),
                    lambda g, e, s, shift=shift: (g + shift, e, 0, 0, 0),
                )
            )
            out_shape.append(
                jax.ShapeDtypeStruct((lead, experts, number, size, columns), bf16)
            )
    in_specs = [pl.BlockSpec(v.shape, lambda g, e, s: (0, 0)) for v in small]
    in_specs.append(
        pl.BlockSpec(
            (depth, None, 2, width),
            lambda g, e, s: (0, e, 0, s[0] ^ (outer ^ mask_of(g, tp_masks[1:]))),
        )
    )
    operands = [tp_index.reshape(1)] + small + [weight]
    if addend is not None:
        operands.append(addend)
        in_specs.append(
            pl.BlockSpec((None, None, 2, count, width), lambda g, e, s: (g, e, 0, 0, 0))
        )
    aliases = {}
    for target, value in into:
        aliases[len(operands)] = target
        operands.append(value)
        in_specs.append(pl.BlockSpec(memory_space=pl.ANY))
    return pl.pallas_call(
        body,
        grid_spec=pltpu.PrefetchScalarGridSpec(
            num_scalar_prefetch=1,
            grid=(blocks, experts),
            in_specs=in_specs,
            out_specs=out_specs,
            scratch_shapes=[pltpu.VMEM((2 * count, 2 * depth), bf16)],
        ),
        out_shape=out_shape,
        input_output_aliases=aliases,
        interpret=INTERPRET,
        name="pair_matmul",
    )(*operands)


def core_split(source_of, weight, tp_index, tp_masks, core_mask, pieces, between=None):
    width = weight.shape[3] >> (len(tp_masks) + 1)
    whole = [((0, 1), 0, width, None)]
    send = {}
    token = []
    for half in (1, 0):
        source = source_of(token)
        send[half] = pair_matmul(
            source, weight, tp_index, tp_masks, core_mask, half, whole
        )[0]
        token = [send[half]]
        if between is not None:
            token = between(1 - half, token)
    got = {half: swap_flat(send[half], core_mask) for half in (1, 0)}
    first = pair_matmul(source_of(token), weight, tp_index, tp_masks, 0, 1, pieces, got[1])
    token = [first[0]]
    if between is not None:
        token = between(2, token)
    into, place = [], 0
    for piece in pieces:
        if piece[3] is None:
            place += 1
        else:
            into += [(place, first[place]), (place + 1, first[place + 1])]
            place += 2
    second = pair_matmul(
        source_of(token), weight, tp_index, tp_masks, 0, 0, pieces, got[0], into
    )
    halves, place = [], 0
    for piece in pieces:
        if piece[3] is None:
            halves.append((second[place], first[place]))
            place += 1
        else:
            halves.append((second[place], second[place + 1]))
            place += 2
    return halves


def prep_kernel(tokens_ref, out_ref):
    values = tokens_ref[...].astype(f32)
    count, model = values.shape
    scale = lax.rsqrt(jnp.sum(values * values, axis=-1, keepdims=True) / model + epsilon)
    both = jnp.concatenate([values, values * scale], axis=0).astype(bf16)
    for block in range(model // LANES):
        out_ref[2 * count * block : 2 * count * (block + 1), :] = both[
            :, LANES * block : LANES * (block + 1)
        ]


def prepare(tokens, devices):
    count, model = tokens.shape
    if model == devices * LANES:
        return pl.pallas_call(
            prep_kernel,
            out_shape=jax.ShapeDtypeStruct((2 * count * devices, LANES), bf16),
            interpret=INTERPRET,
            name="prepare",
        )(tokens)
    values = tokens.astype(f32)
    scale = lax.rsqrt(jnp.mean(values * values, axis=-1, keepdims=True) + epsilon)
    both = jnp.stack([tokens, (values * scale).astype(bf16)])
    both = both.reshape(2 * count, devices, model // devices).transpose(1, 0, 2)
    return both.reshape(2 * count * devices, model // devices)


def out_kernel(index_ref, start_ref, gated_ref, weight_ref, out_ref):
    @pl.when(pl.program_id(0) == 0)
    def _():
        out_ref[...] = start_ref[...].astype(f32)

    out_ref[...] += jnp.dot(gated_ref[...], weight_ref[...], preferred_element_type=f32)


def out_matmul(start, gated, weight, tp_index, tp_masks, fixed):
    blocks, rows, width = gated.shape
    columns = weight.shape[1]
    grid_spec = pltpu.PrefetchScalarGridSpec(
        num_scalar_prefetch=1,
        grid=(blocks,),
        in_specs=[
            pl.BlockSpec(start.shape, lambda g, s: (0, 0)),
            pl.BlockSpec((None, rows, width), lambda g, s: (g, 0, 0)),
            pl.BlockSpec((width, columns), lambda g, s: (s[0] ^ (fixed ^ mask_of(g, tp_masks)), 0)),
        ],
        out_specs=pl.BlockSpec((rows, columns), lambda g, s: (0, 0)),
    )
    return pl.pallas_call(
        out_kernel,
        grid_spec=grid_spec,
        out_shape=jax.ShapeDtypeStruct((rows, columns), f32),
        interpret=INTERPRET,
        name="out_matmul",
    )(tp_index.reshape(1), start, gated, weight)


def chains_of(halves, orders, tp_masks, rep_masks):
    chains = []
    for (keep, send), order in zip(halves, orders):
        tp_left = [m for m in tp_masks if m != order[0]]
        rep_left = [m for m in rep_masks if m != order[0]]
        shape = (2,) * len(tp_left) + keep.shape[1:3] + (2,) * len(rep_left)
        shape = shape + (keep.shape[3] >> len(rep_left), keep.shape[4])
        names = tp_left + [None, None] + rep_left
        chains.append((keep.reshape(shape), send.reshape(shape), names, order))
    return chains


def swap_flat(value, mask):
    return swap(value.reshape((-1,) + value.shape[-2:]), mask).reshape(value.shape)


def shards(
    tokens,
    conv_state,
    ssm_state,
    norm_gains,
    conv_weight,
    conv_skip,
    step_bias,
    decay_log,
    input_proj,
    select_proj,
    step_proj,
    output_proj,
    router,
    expert_proj,
    expert_ids,
):
    tp_count = lax.axis_size("tp")
    rep_count = lax.axis_size("rep")
    devices = tp_count * rep_count
    tp_index = lax.axis_index("tp").astype(jnp.int32)
    rep_index = lax.axis_index("rep").astype(jnp.int32)
    tp_bits = [1 << k for k in range(tp_count.bit_length() - 1)]
    rep_bits = [1 << k for k in range(rep_count.bit_length() - 1)]
    core_mask = tp_bits[0]
    if len(rep_bits) > 2:
        rep_bits[-1] = rep_bits[-1] | rep_bits[-2]
    rows_masks = list(rep_bits)
    rows_joint = [m * tp_count for m in rows_masks]
    far = list(reversed(rows_joint))
    tp_rest = tp_bits[1:]
    tp_masks = list(reversed(tp_rest))
    near = [far[-1]] + tp_rest
    groups = [far[:-1][k : k + 2] for k in range(0, len(far) - 1, 2)]
    groups += [near[k : k + 2] for k in range(0, len(near), 2)]
    base_order = tp_masks + rows_joint
    head = tp_masks[:1] + rows_joint[:2]
    tail = tp_masks[1:] + rows_joint[2:]

    def order_of(k):
        return head[k % 3 :] + head[: k % 3] + tail

    tok_dev, model = tokens.shape
    feature_dev = model // devices
    inner_dev = ssm_state.shape[2]
    state_count = ssm_state.shape[1]
    per_rep = tok_dev * tp_count
    total_tokens = tok_dev * devices

    both = prepare(tokens, devices)

    params, select_own, step_own = after(
        (
            jnp.concatenate([conv_weight, conv_skip, step_bias[None], decay_log], axis=0),
            select_proj.T[None],
            step_proj,
        ),
        both,
    )
    taps = conv_weight.shape[0]
    params_dev, channel_dev = params.shape
    homes = [(b, (b % rep_count) * tp_count + b // rep_count) for b in range(devices)]
    step_rows = step_proj.shape[0]
    params = lax.ppermute(params, AXES, homes)
    params_rows = -(-params_dev * channel_dev // inner_dev)
    padded_rows = -(-params_rows // step_rows) * step_rows
    select_rel = gather_stage(select_own, far[:1])
    step_parts = []
    for d in range(tp_count):
        piece = lax.dynamic_slice_in_dim(step_own, (tp_index ^ d) * inner_dev, inner_dev, 1)
        step_parts.append(swap(piece, d) if d else piece)
    flat = params.reshape(-1)
    flat = jnp.pad(flat, (0, padded_rows * inner_dev - flat.shape[0]))
    step_rel = jnp.concatenate(step_parts + [flat.reshape(padded_rows, inner_dev)])[None]

    row = jnp.arange(total_tokens, dtype=jnp.int32)
    absolute_row = (rep_index ^ mask_of(row // per_rep, rows_masks)) * per_rep + row % per_rep
    to_rel = (absolute_row[:, None] == row[None, :]).astype(bf16)
    spread_row = (absolute_row // tok_dev) * (2 * tok_dev) + absolute_row % tok_dev
    column = jnp.arange(2 * total_tokens, dtype=jnp.int32)
    pick_in = (spread_row[:, None] == column[None, :]).astype(bf16)
    pick_unit = (spread_row[:, None] + tok_dev == column[None, :]).astype(bf16)
    gains = norm_gains.astype(f32)

    spread = lax.all_to_all(both, AXES, split_axis=0, concat_axis=0, tiled=True)
    step_order = far[:1] + far[-1:] + far[-2:0:-1]
    step_rel = gather_stage(step_rel, step_order[:1])
    select_rel = gather_stage(after(select_rel, spread), far[1:2])

    later = {}

    def between(call, token):
        if call == 0:
            later["step"] = gather_stage(after(step_rel, token), step_order[1:2])
        if call == 2:
            later["select"], later["step"] = after((select_rel, later["step"]), token)
            token = token + [later["select"], later["step"]]
            for mask in far[2:]:
                later["select"] = gather_stage(later["select"], [mask])
            for mask in step_order[2:]:
                later["step"] = gather_stage(later["step"], [mask])
        return token

    halves = core_split(
        lambda token: (after(spread, token), pick_unit, gains[:1]),
        input_proj[:, None],
        tp_index,
        tp_masks,
        core_mask,
        [((0,), 0, inner_dev, None), ((1,), 0, inner_dev, None)],
        between,
    )
    block_in = jnp.dot(pick_in, spread, preferred_element_type=f32)

    projected = scatter_bits(
        chains_of(halves, [base_order] * 2, tp_masks, rows_joint),
        lambda step, sends, gots: gots,
    )
    conv_input, gate_z = [part[0, 0] for part in projected]
    select_rel = later["select"]
    step_rel = later["step"]

    step_masks = [m // tp_count for m in reversed(step_order)]
    step_block = step_rows * tp_count + padded_rows
    params_rel = step_rel[:, step_rows * tp_count :].reshape(rep_count, -1)
    params_rel = params_rel[:, : params_dev * channel_dev]
    params_rel = params_rel.reshape(rep_count, params_dev, channel_dev)
    own = index_of(rep_index, step_masks)
    params_all = jnp.concatenate(
        [
            lax.dynamic_index_in_dim(
                params_rel, index_of(r, step_masks) ^ own, 0, keepdims=False
            )
            for r in range(rep_count)
        ],
        axis=-1,
    ).astype(f32)
    conv_taps = params_all[:taps]
    skip_rows = params_all[taps : taps + 2]
    shift_dev = params_all[taps + 2]
    decay_dev = params_all[taps + 3 :]

    history = conv_state.astype(f32)
    conv_mix = (
        jnp.sum(conv_taps[:-1, None, :] * history, axis=0)
        + conv_taps[-1] * conv_input
        + skip_rows[0]
    )
    conv_next = jnp.concatenate([conv_state[1:], conv_input.astype(bf16)[None]], axis=0)
    activated = jax.nn.silu(conv_mix)
    select_cols = select_rel.shape[0] * select_rel.shape[1]
    select_part = lax.dot_general(
        activated.astype(bf16),
        select_rel.reshape(select_cols, inner_dev),
        (((1,), (1,)), ((), ())),
        preferred_element_type=f32,
    )
    selected = select_part
    for d in range(1, tp_count):
        selected = selected + swap(select_part, d)
    selected = selected.astype(bf16)
    step_rank = devices * step_rows
    column = jnp.arange(select_cols, dtype=jnp.int32)
    per_block = select_proj.shape[1]
    total_rank = rep_count * step_block
    absolute_col = (rep_index ^ mask_of(column // per_block, rows_masks)) * per_block + (
        column % per_block
    )
    rank = jnp.arange(total_rank, dtype=jnp.int32)
    rank_rep = rep_index ^ mask_of(rank // step_block, step_masks)
    inside = rank % step_block
    wanted = (rank_rep * tp_count + (tp_index ^ (inside // step_rows))) * step_rows
    wanted = jnp.where(inside < step_rows * tp_count, wanted + inside % step_rows, -1)
    wanted = jnp.concatenate([wanted, jnp.arange(step_rank, select_cols, dtype=jnp.int32)])
    reorder = (absolute_col[:, None] == wanted[None, :]).astype(bf16)
    selected = jnp.dot(selected, reorder, preferred_element_type=f32)
    step_low = selected[:, :total_rank].astype(bf16)
    input_map = selected[:, total_rank : total_rank + state_count]
    output_map = selected[:, total_rank + state_count :]
    step_rel = step_rel.reshape(total_rank, inner_dev)
    step_size = jax.nn.softplus(
        jnp.dot(step_low, step_rel, preferred_element_type=f32) + shift_dev
    )
    decay_rate = -jnp.exp(decay_dev)
    factor = jnp.exp(step_size[:, None, :] * decay_rate[None])
    ssm_next = factor * ssm_state + (step_size * activated)[:, None, :] * input_map[:, :, None]
    readout = jnp.sum(ssm_next * output_map[:, :, None], axis=1) + skip_rows[1] * activated
    gated_out = (readout * jax.nn.silu(gate_z)).astype(bf16)

    gated = gated_out[None]
    for group in groups:
        gated = gather_stage(gated.reshape((-1,) + gated_out.shape), group)
    gated = gated.reshape(tp_count // 2, total_tokens, inner_dev)
    gated_got = swap_flat(gated, core_mask)
    residual = out_matmul(block_in, gated, output_proj, tp_index, tp_masks, 0)
    residual = out_matmul(residual, gated_got, output_proj, tp_index, tp_masks, core_mask)

    pieces, orders, first = [], [], 0
    for k, columns in enumerate(color_widths(expert_proj.shape[3] // tp_count)):
        orders.append(order_of(k))
        split = None if k % 3 == 0 else rows_joint.index(orders[k][0])
        pieces.append(((0, 1), first, columns, split))
        first += columns
    halves = core_split(
        lambda token: (after(residual, token), None, gains[1:]),
        expert_proj,
        tp_index,
        tp_masks,
        core_mask,
        pieces,
    )
    tied = {}

    def hook(step, sends, gots):
        if step == 0:
            tied["residual"] = after(residual, sends)
        if step == min(2, len(base_order) - 1):
            tied["late"] = sends
        return gots

    summed = scatter_bits(chains_of(halves, orders, tp_masks, rows_joint), hook, True)[0]
    residual = tied["residual"]

    rows_moe = (residual * gains[1]).astype(bf16)
    expert_total = router.shape[1]
    partial = jnp.concatenate(
        [
            jnp.dot(rows_moe, router, preferred_element_type=f32),
            jnp.sum(residual * residual, axis=-1, keepdims=True),
        ],
        axis=-1,
    )
    high = lax.reduce_precision(partial, 8, 7)
    low = partial - high
    half = LANES // 2
    mine = (row[:, None] - tp_index * tok_dev == jnp.arange(tok_dev)[None, :]).astype(f32)
    ids_rows = jnp.dot(mine, expert_ids.astype(f32), precision=lax.Precision.HIGHEST)
    facts = jnp.concatenate([high, low, ids_rows], axis=-1).astype(bf16)
    facts = jnp.pad(facts, ((0, 0), (0, half - facts.shape[1])))
    outgoing = jnp.concatenate([residual.astype(bf16), facts], axis=-1)
    outgoing = lax.dot_general(
        to_rel, outgoing, (((0,), (0,)), ((), ())), preferred_element_type=f32
    ).astype(bf16)
    out_rows = outgoing[:, :feature_dev].reshape(devices, tok_dev * feature_dev)
    out_facts = outgoing[:, feature_dev:].reshape(rep_count, 1, per_rep * half)
    out_facts = jnp.broadcast_to(out_facts, (rep_count, tp_count, per_rep * half))
    out_facts = out_facts.reshape(devices, per_rep * half)
    outgoing = jnp.concatenate([out_rows, out_facts], axis=-1)
    incoming = lax.all_to_all(outgoing, AXES, split_axis=0, concat_axis=0, tiled=True)
    incoming = after(incoming, tied["late"])
    mamba_out = incoming[:, : tok_dev * feature_dev].reshape(devices, tok_dev, feature_dev)
    mamba_out = mamba_out.transpose(1, 0, 2).reshape(tok_dev, model)
    facts = incoming[:, tok_dev * feature_dev :].astype(f32).sum(axis=0).reshape(per_rep, half)
    ids_all = facts[:, 2 * (expert_total + 1) : 2 * (expert_total + 1) + 2].astype(jnp.int32)
    facts = facts[:, : expert_total + 1] + facts[:, expert_total + 1 : 2 * (expert_total + 1)]
    moe_scale = lax.rsqrt(facts[:, expert_total:] / model + epsilon)
    logits = facts[:, :expert_total] * moe_scale

    choose = (
        ids_all[:, :, None] == jnp.arange(expert_total, dtype=jnp.int32)[None, None, :]
    ).astype(f32)
    picked = jnp.sum(choose * logits[:, None, :], axis=2)
    first_gate = jax.nn.sigmoid(picked[:, 0] - picked[:, 1])
    second_gate = jax.nn.sigmoid(picked[:, 1] - picked[:, 0])
    window_count = expert_proj.shape[1]
    window = jnp.arange(window_count, dtype=jnp.int32)
    names_first = ids_all[:, 0:1] == window[None, :]
    names_second = ids_all[:, 1:2] == window[None, :]
    zero = jnp.zeros((), f32)
    gate_w = jnp.where(names_first, first_gate[:, None], zero) + jnp.where(
        names_second, second_gate[:, None], zero
    )
    gate_w = gate_w.astype(bf16).astype(f32)
    routed = (names_first | names_second).astype(jnp.int32).reshape(tp_count, tok_dev, window_count)
    position = jnp.cumsum(routed, axis=1) - routed
    slot_of = (position[..., None] == jnp.arange(CAPACITY, dtype=jnp.int32)) & (
        routed[..., None] > 0
    )
    gate_up = summed * moe_scale[None, None]
    hidden = gate_w.T[:, :, None] * jax.nn.silu(gate_up[:, 0]) * gate_up[:, 1]
    hidden = hidden.astype(bf16).reshape(window_count, tp_count, tok_dev, -1)
    expert_hidden = jnp.einsum(
        "jtec,ejtf->jecf", slot_of.astype(bf16), hidden, preferred_element_type=f32
    ).astype(bf16)
    expert_hidden = expert_hidden.reshape(tp_count * window_count * CAPACITY, -1)
    return (mamba_out, conv_next, ssm_next, expert_hidden)


def solution(mesh):
    in_specs = (
        P(("rep", "tp"), None),
        P(None, "rep", "tp"),
        P("rep", None, "tp"),
        P(None, ("rep", "tp")),
        P(None, ("rep", "tp")),
        P(None, ("rep", "tp")),
        P(("rep", "tp")),
        P(None, ("rep", "tp")),
        P(("rep", "tp"), None, None),
        P("tp", "rep"),
        P(("rep", "tp"), None),
        P(None, ("rep", "tp")),
        P(("rep", "tp"), None),
        P(("rep", "tp"), None, None, None),
        P(("rep", "tp"), None),
    )
    out_specs = (P(("rep", "tp"), None), P(None, "rep", "tp"), P("rep", None, "tp"), P("rep", "tp"))
    return jax.shard_map(shards, mesh=mesh, in_specs=in_specs, out_specs=out_specs, check_vma=False)
```

```python
import jax
import jax.numpy as jnp
from jax import lax
from jax.experimental import pallas as pl
from jax.experimental.pallas import tpu as pltpu
from jax.sharding import PartitionSpec as P

CAPACITY = 2
LANES = 128
INTERPRET = False
AXES = ("rep", "tp")
epsilon = 1e-05
bf16 = jnp.bfloat16
f32 = jnp.float32


def swap(value, mask):
    count = lax.axis_size(AXES)
    return lax.ppermute(value, AXES, [(i, i ^ mask) for i in range(count)])


def mask_of(index, masks):
    total = 0
    for k, mask in enumerate(reversed(masks)):
        total = total ^ (((index >> k) & 1) * mask)
    return total


def index_of(mask, masks):
    count = 1 << len(masks)
    table = {mask_of(i, masks): i for i in range(count)}
    if isinstance(mask, int):
        return table[mask]
    total = 0
    for k in range(len(masks)):
        total = total ^ (((mask >> k) & 1) * table[1 << k])
    return total


def after(value, *others):
    return lax.optimization_barrier((value, others))[0]


def gather_stage(value, group):
    parts = []
    for combo in range(1 << len(group)):
        mask = mask_of(combo, list(reversed(group)))
        parts.append(swap(value, mask) if mask else value)
    return jnp.stack(parts).reshape((-1,) + value.shape[1:])


def gather_last(value, masks):
    for mask in masks[:-1]:
        value = gather_stage(value, [mask])
    return [value, swap(value, masks[-1])]


def take_bit(value, axis, which):
    return lax.index_in_dim(value, which, axis, keepdims=False)


def add_bf(left, right):
    return (left.astype(f32) + right.astype(f32)).astype(bf16)


def scatter_bits(chains, hook, merge=False):
    chains = [list(chain) for chain in chains]
    for step in range(len(chains[0][3])):
        sends = []
        gots = []
        for chain in chains:
            keep, send, names, order = chain
            if step:
                axis = names.index(order[step])
                left, right = keep
                send = add_bf(take_bit(left, axis, 1), take_bit(right, axis, 1))
                keep = add_bf(take_bit(left, axis, 0), take_bit(right, axis, 0))
                chain[2] = names[:axis] + names[axis + 1 :]
            sends.append(send.reshape((-1,) + send.shape[-2:]))
            chain[0] = keep
        if merge and step == len(chains[0][3]) - 1:
            chains[0][0] = jnp.concatenate([chain[0] for chain in chains], axis=-1)
            chains = chains[:1]
            sends = [jnp.concatenate(sends, axis=-1)]
        for chain, flat in zip(chains, sends):
            gots.append(swap(flat, chain[3][step]).reshape(chain[0].shape))
        gots = hook(step, sends, gots)
        for chain, got in zip(chains, gots):
            chain[0] = (chain[0], got)
    return [left.astype(f32) + right.astype(f32) for (left, right), *_ in chains]


def color_widths(width):
    blocks = width // LANES
    if blocks < 3 or width % LANES:
        return [width]
    base = blocks // 3
    extra = blocks - 3 * base
    return [(base + (k < extra)) * LANES for k in range(3)]


def split_at(rows, position):
    half = rows >> (position + 1)
    return [
        [(o * 2 * half + bit * half, half) for o in range(1 << position)] for bit in range(2)
    ]


def pair_matmul(rows, weight, tp_index, tp_masks, fixed, half, pieces, addend=None, into=None):
    source, pick, gain = rows
    depth, experts = weight.shape[0], weight.shape[1]
    count = source.shape[0] if pick is None else pick.shape[0]
    blocks = 1 << (len(tp_masks) - 1)
    width = weight.shape[3] // (4 * blocks)
    outer = fixed ^ (tp_masks[0] if half else 0)
    small = [source] + ([] if pick is None else [pick]) + [gain]
    into = [] if into is None else into

    def body(index_ref, *refs):
        refs = list(refs)
        rows_ref = refs.pop()
        source_ref = refs.pop(0)
        pick_ref = None if pick is None else refs.pop(0)
        gain_ref = refs.pop(0)
        weight_ref = refs.pop(0)
        addend_ref = None if addend is None else refs.pop(0)
        out_refs = refs[len(into) :]

        @pl.when((pl.program_id(0) == 0) & (pl.program_id(1) == 0))
        def _():
            picked = source_ref[...]
            if pick_ref is not None:
                picked = jnp.dot(pick_ref[...], picked, preferred_element_type=f32)
            scaled = (picked * gain_ref[...]).astype(bf16)
            row = lax.broadcasted_iota(jnp.int32, (depth, 2 * depth), 0)
            column = lax.broadcasted_iota(jnp.int32, (depth, 2 * depth), 1)
            for x in range(2):
                place = jnp.where(column == 2 * row + x, 1.0, 0.0).astype(bf16)
                wide = jnp.dot(scaled, place, preferred_element_type=f32)
                rows_ref[x * count : (x + 1) * count, :] = wide.astype(bf16)

        result = jnp.dot(
            rows_ref[...],
            weight_ref[...].reshape(2 * depth, width),
            preferred_element_type=f32,
        )
        if addend_ref is not None:
            result = result + addend_ref[...].reshape(2 * count, width).astype(f32)
        result = result.astype(bf16)
        targets = iter(out_refs)
        for planes, first, columns, split in pieces:
            groups = [[(0, count)]] if split is None else split_at(count, split)
            for group in groups:
                target = next(targets)
                for k, plane in enumerate(planes):
                    base = 0
                    for start, size in group:
                        low = plane * count + start
                        target[k, base : base + size, :] = result[
                            low : low + size, first : first + columns
                        ]
                        base += size

    out_specs, out_shape = [], []
    for planes, _, columns, split in pieces:
        number = len(planes)
        if split is None:
            outs, lead, shift, size = 1, blocks, 0, count
        else:
            outs, lead, shift, size = 2, 2 * blocks, half * blocks, count // 2
        for _ in range(outs):
            out_specs.append(
                pl.BlockSpec(
                    (None, None, number, size, columns),
                    lambda g, e, s, shift=shift: (g + shift, e, 0, 0, 0),
                )
            )
            out_shape.append(
                jax.ShapeDtypeStruct((lead, experts, number, size, columns), bf16)
            )
    in_specs = [pl.BlockSpec(v.shape, lambda g, e, s: (0, 0)) for v in small]
    in_specs.append(
        pl.BlockSpec(
            (depth, None, 2, width),
            lambda g, e, s: (0, e, 0, s[0] ^ (outer ^ mask_of(g, tp_masks[1:]))),
        )
    )
    operands = [tp_index.reshape(1)] + small + [weight]
    if addend is not None:
        operands.append(addend)
        in_specs.append(
            pl.BlockSpec((None, None, 2, count, width), lambda g, e, s: (g, e, 0, 0, 0))
        )
    aliases = {}
    for target, value in into:
        aliases[len(operands)] = target
        operands.append(value)
        in_specs.append(pl.BlockSpec(memory_space=pl.ANY))
    return pl.pallas_call(
        body,
        grid_spec=pltpu.PrefetchScalarGridSpec(
            num_scalar_prefetch=1,
            grid=(blocks, experts),
            in_specs=in_specs,
            out_specs=out_specs,
            scratch_shapes=[pltpu.VMEM((2 * count, 2 * depth), bf16)],
        ),
        out_shape=out_shape,
        input_output_aliases=aliases,
        interpret=INTERPRET,
        name="pair_matmul",
    )(*operands)


def core_split(source_of, weight, tp_index, tp_masks, core_mask, pieces, between=None):
    width = weight.shape[3] >> (len(tp_masks) + 1)
    whole = [((0, 1), 0, width, None)]
    send = {}
    token = []
    for half in (1, 0):
        source = source_of(token)
        send[half] = pair_matmul(
            source, weight, tp_index, tp_masks, core_mask, half, whole
        )[0]
        token = [send[half]]
        if between is not None:
            token = between(1 - half, token)
    got = {half: swap_flat(send[half], core_mask) for half in (1, 0)}
    first = pair_matmul(source_of(token), weight, tp_index, tp_masks, 0, 1, pieces, got[1])
    token = [first[0]]
    if between is not None:
        token = between(2, token)
    into, place = [], 0
    for piece in pieces:
        if piece[3] is None:
            place += 1
        else:
            into += [(place, first[place]), (place + 1, first[place + 1])]
            place += 2
    second = pair_matmul(
        source_of(token), weight, tp_index, tp_masks, 0, 0, pieces, got[0], into
    )
    halves, place = [], 0
    for piece in pieces:
        if piece[3] is None:
            halves.append((second[place], first[place]))
            place += 1
        else:
            halves.append((second[place], second[place + 1]))
            place += 2
    return halves


def prep_kernel(tp_count, tokens_ref, step_ref, out_ref):
    values = tokens_ref[...].astype(f32)
    count, model = values.shape
    rows = step_ref.shape[0]
    devices = model // LANES
    sub = step_ref.shape[1] // devices
    scale = lax.rsqrt(jnp.sum(values * values, axis=-1, keepdims=True) / model + epsilon)
    filler = jnp.zeros((rows - 2 * count, model), f32)
    both = jnp.concatenate([values, values * scale, filler], axis=0).astype(bf16)
    for device in range(devices):
        low = LANES * device
        out_ref[device, :rows, :] = both[:, low : low + LANES]
        block = (device % tp_count) * (devices // tp_count) + device // tp_count
        for part in range(sub // LANES):
            low = sub * block + LANES * part
            high = rows * (part + 1)
            out_ref[device, high : high + rows, :] = step_ref[:, low : low + LANES]


def exchange(tokens, step_proj, tp_count, rep_count):
    count, model = tokens.shape
    rows, inner = step_proj.shape
    devices = tp_count * rep_count
    sub = inner // devices
    each = jnp.arange(devices * count, dtype=jnp.int32)
    if model == devices * LANES and sub % LANES == 0 and rows % 8 == 0 and rows >= 2 * count:
        high = rows * (1 + sub // LANES)
        out = pl.pallas_call(
            lambda *refs: prep_kernel(tp_count, *refs),
            out_shape=jax.ShapeDtypeStruct((devices, high, LANES), bf16),
            interpret=INTERPRET,
            name="prepare",
        )(tokens, step_proj)
        out = out.reshape(devices * high, LANES)
        ready = out
        out = lax.all_to_all(out, AXES, split_axis=0, concat_axis=0, tiled=True)
        step = out.reshape(devices, high, LANES)[:, rows:]
        step = step.reshape(devices, sub // LANES, rows, LANES).transpose(0, 2, 1, 3)
        place = (each // count) * high + each % count
        return ready, out, place, step.reshape(devices * rows, sub)
    values = tokens.astype(f32)
    scale = lax.rsqrt(jnp.mean(values * values, axis=-1, keepdims=True) + epsilon)
    both = jnp.stack([tokens, (values * scale).astype(bf16)])
    both = both.reshape(2 * count, devices, model // devices).transpose(1, 0, 2)
    both = both.reshape(2 * count * devices, model // devices)
    step = step_proj.reshape(rows, tp_count, rep_count, sub).transpose(2, 1, 0, 3)
    step = step.reshape(devices, rows * sub)
    step = lax.all_to_all(step, AXES, split_axis=0, concat_axis=0, tiled=True)
    out = lax.all_to_all(both, AXES, split_axis=0, concat_axis=0, tiled=True)
    place = (each // count) * (2 * count) + each % count
    return both, out, place, step.reshape(devices * rows, sub)


def out_matmul(start, gated, weight, tp_index, tp_masks, fixed):
    blocks, rows, width = gated.shape
    columns = weight.shape[1]
    start = list(start) if isinstance(start, tuple) else [start]

    def body(index_ref, *refs):
        gated_ref, weight_ref, out_ref = refs[len(start) :]

        @pl.when(pl.program_id(0) == 0)
        def _():
            if len(start) == 1:
                out_ref[...] = refs[0][...]
            else:
                out_ref[...] = jnp.dot(refs[0][...], refs[1][...], preferred_element_type=f32)

        out_ref[...] += jnp.dot(gated_ref[...], weight_ref[...], preferred_element_type=f32)

    grid_spec = pltpu.PrefetchScalarGridSpec(
        num_scalar_prefetch=1,
        grid=(blocks,),
        in_specs=[pl.BlockSpec(v.shape, lambda g, s: (0, 0)) for v in start]
        + [
            pl.BlockSpec((None, rows, width), lambda g, s: (g, 0, 0)),
            pl.BlockSpec((width, columns), lambda g, s: (s[0] ^ (fixed ^ mask_of(g, tp_masks)), 0)),
        ],
        out_specs=pl.BlockSpec((rows, columns), lambda g, s: (0, 0)),
    )
    return pl.pallas_call(
        body,
        grid_spec=grid_spec,
        out_shape=jax.ShapeDtypeStruct((rows, columns), f32),
        interpret=INTERPRET,
        name="out_matmul",
    )(tp_index.reshape(1), *start, gated, weight)


def chains_of(halves, orders, tp_masks, rep_masks):
    chains = []
    for (keep, send), order in zip(halves, orders):
        tp_left = [m for m in tp_masks if m != order[0]]
        rep_left = [m for m in rep_masks if m != order[0]]
        shape = (2,) * len(tp_left) + keep.shape[1:3] + (2,) * len(rep_left)
        shape = shape + (keep.shape[3] >> len(rep_left), keep.shape[4])
        names = tp_left + [None, None] + rep_left
        chains.append((keep.reshape(shape), send.reshape(shape), names, order))
    return chains


def swap_flat(value, mask):
    return swap(value.reshape((-1,) + value.shape[-2:]), mask).reshape(value.shape)


def shards(
    tokens,
    conv_state,
    ssm_state,
    norm_gains,
    conv_weight,
    conv_skip,
    step_bias,
    decay_log,
    input_proj,
    select_proj,
    step_proj,
    output_proj,
    router,
    expert_proj,
    expert_ids,
):
    tp_count = lax.axis_size("tp")
    rep_count = lax.axis_size("rep")
    devices = tp_count * rep_count
    tp_index = lax.axis_index("tp").astype(jnp.int32)
    rep_index = lax.axis_index("rep").astype(jnp.int32)
    tp_bits = [1 << k for k in range(tp_count.bit_length() - 1)]
    rep_bits = [1 << k for k in range(rep_count.bit_length() - 1)]
    core_mask = tp_bits[0]
    if len(rep_bits) > 2:
        rep_bits[-1] = rep_bits[-1] | rep_bits[-2]
    rows_masks = list(rep_bits)
    rows_joint = [m * tp_count for m in rows_masks]
    far = list(reversed(rows_joint))
    tp_rest = tp_bits[1:]
    tp_masks = list(reversed(tp_rest))
    near = [far[-1]] + tp_rest
    groups = [far[:-1][k : k + 2] for k in range(0, len(far) - 1, 2)]
    groups += [near[k : k + 2] for k in range(0, len(near), 2)]
    base_order = tp_masks + rows_joint
    head = tp_masks[:1] + rows_joint[:2]
    tail = tp_masks[1:] + rows_joint[2:]

    def order_of(k):
        return head[k % 3 :] + head[: k % 3] + tail

    tok_dev, model = tokens.shape
    feature_dev = model // devices
    inner_dev = ssm_state.shape[2]
    state_count = ssm_state.shape[1]
    per_rep = tok_dev * tp_count
    total_tokens = tok_dev * devices

    ready, spread, place, step_block = exchange(tokens, step_proj, tp_count, rep_count)

    params, select_own = after(
        (
            jnp.concatenate([conv_weight, conv_skip, step_bias[None], decay_log], axis=0),
            jnp.pad(select_proj.T, ((0, -select_proj.shape[1] % 8), (0, 0)))[None],
        ),
        ready,
    )
    taps = conv_weight.shape[0]
    params_dev, channel_dev = params.shape
    homes = [(b, (b % rep_count) * tp_count + b // rep_count) for b in range(devices)]
    params = lax.ppermute(params, AXES, homes)
    step_rank = step_block.shape[0]
    params = jnp.pad(params, ((0, -params_dev % 8), (0, 0)))
    total_rank = step_rank + params.shape[0]
    step_rel = jnp.concatenate([step_block, params])[None]
    select_rel = gather_stage(select_own, far[:1])

    row = jnp.arange(total_tokens, dtype=jnp.int32)
    absolute_row = (rep_index ^ mask_of(row // per_rep, rows_masks)) * per_rep + row % per_rep
    to_rel = (absolute_row[:, None] == row[None, :]).astype(bf16)
    spread_row = jnp.sum(
        jnp.where(absolute_row[:, None] == row[None, :], place[None, :], 0), axis=1
    )
    column = jnp.arange(spread.shape[0], dtype=jnp.int32)
    pick_in = (spread_row[:, None] == column[None, :]).astype(bf16)
    pick_unit = (spread_row[:, None] + tok_dev == column[None, :]).astype(bf16)
    gains = norm_gains.astype(f32)

    step_order = far[:1] + far[-1:] + far[-2:0:-1]
    step_rel = gather_stage(step_rel, step_order[:1])
    select_rel = gather_stage(after(select_rel, spread), far[1:2])

    later = {}

    def between(call, token):
        if call == 0:
            later["step"] = gather_stage(after(step_rel, token), step_order[1:2])
        if call == 2:
            later["select"], later["step"] = after((select_rel, later["step"]), token)
            token = token + [later["select"], later["step"]]
            later["select"] = gather_last(later["select"], far[2:])
            later["step"] = gather_last(later["step"], step_order[2:])
        return token

    halves = core_split(
        lambda token: (after(spread, token), pick_unit, gains[:1]),
        input_proj[:, None],
        tp_index,
        tp_masks,
        core_mask,
        [((0,), 0, inner_dev, None), ((1,), 0, inner_dev, None)],
        between,
    )

    def fetched(step, sends, gots):
        return gots

    projected = scatter_bits(
        chains_of(halves, [base_order] * 2, tp_masks, rows_joint),
        fetched,
    )
    conv_input, gate_z = [part[0, 0] for part in projected]
    select_rel = later["select"]
    step_rel = later["step"]

    step_masks = [m // tp_count for m in reversed(step_order)]
    params_rel = jnp.concatenate(
        [part[:, step_rank : step_rank + params_dev] for part in step_rel]
    )
    own = index_of(rep_index, step_masks)

    def in_channel_order(parts):
        return jnp.concatenate(
            [
                lax.dynamic_index_in_dim(parts, index_of(r, step_masks) ^ own, 0, keepdims=False)
                for r in range(rep_count)
            ],
            axis=-1,
        )

    params_all = lax.optimization_barrier(in_channel_order(params_rel)).astype(f32)
    conv_taps = params_all[:taps]
    skip_rows = params_all[taps : taps + 2]
    shift_dev = params_all[taps + 2]
    decay_dev = params_all[taps + 3 :]

    history = conv_state.astype(f32)
    conv_mix = (
        jnp.sum(conv_taps[:-1, None, :] * history, axis=0)
        + conv_taps[-1] * conv_input
        + skip_rows[0]
    )
    conv_next = jnp.concatenate([conv_state[1:], conv_input.astype(bf16)[None]], axis=0)
    activated = jax.nn.silu(conv_mix)
    per_block = select_rel[0].shape[1]
    select_cols = rep_count * per_block
    activated_bf = activated.astype(bf16)
    select_part = jnp.concatenate(
        [
            lax.dot_general(
                activated_bf,
                part.reshape(select_cols // 2, inner_dev),
                (((1,), (1,)), ((), ())),
                preferred_element_type=f32,
            )
            for part in select_rel
        ],
        axis=-1,
    )
    selected = select_part
    for d in range(1, tp_count):
        selected = selected + swap(select_part, d)
    selected = selected.astype(bf16)
    column = jnp.arange(select_cols, dtype=jnp.int32)
    held = select_proj.shape[1]
    inside = column % per_block
    absolute_col = (rep_index ^ mask_of(column // per_block, rows_masks)) * held + inside
    absolute_col = jnp.where(inside < held, absolute_col, -2)
    wanted = jnp.arange(total_rank, dtype=jnp.int32)
    wanted = jnp.where(wanted < step_rank, wanted, -1)
    wanted = jnp.concatenate([wanted, jnp.arange(step_rank, rep_count * held, dtype=jnp.int32)])
    reorder = (absolute_col[:, None] == wanted[None, :]).astype(bf16)
    selected = jnp.dot(selected, reorder, preferred_element_type=f32)
    step_low = selected[:, :total_rank].astype(bf16)
    input_map = selected[:, total_rank : total_rank + state_count]
    output_map = selected[:, total_rank + state_count :]
    step_parts = jnp.concatenate(
        [
            jnp.einsum("sk,dkc->dsc", step_low, part, preferred_element_type=f32)
            for part in step_rel
        ]
    )
    step_size = lax.optimization_barrier(in_channel_order(step_parts))
    step_size = jax.nn.softplus(step_size + shift_dev)
    decay_rate = -jnp.exp(decay_dev)
    factor = jnp.exp(step_size[:, None, :] * decay_rate[None])
    ssm_next = factor * ssm_state + (step_size * activated)[:, None, :] * input_map[:, :, None]
    readout = jnp.sum(ssm_next * output_map[:, :, None], axis=1) + skip_rows[1] * activated
    gated_out = (readout * jax.nn.silu(gate_z)).astype(bf16)

    gated = gated_out[None]
    for level, group in enumerate(groups):
        if level == 1:
            gated, conv_next, ssm_next = lax.optimization_barrier((gated, conv_next, ssm_next))
        gated = gather_stage(gated.reshape((-1,) + gated_out.shape), group)
    gated = gated.reshape(tp_count // 2, total_tokens, inner_dev)
    gated_got = swap_flat(gated, core_mask)
    residual = out_matmul((pick_in, spread), gated, output_proj, tp_index, tp_masks, 0)
    residual = out_matmul(residual, gated_got, output_proj, tp_index, tp_masks, core_mask)

    pieces, orders, first = [], [], 0
    for k, columns in enumerate(color_widths(expert_proj.shape[3] // tp_count)):
        orders.append(order_of(k))
        split = None if k % 3 == 0 else rows_joint.index(orders[k][0])
        pieces.append(((0, 1), first, columns, split))
        first += columns
    halves = core_split(
        lambda token: (after(residual, token), None, gains[1:]),
        expert_proj,
        tp_index,
        tp_masks,
        core_mask,
        pieces,
    )
    tied = {}

    def hook(step, sends, gots):
        if step == 0:
            tied["residual"] = after(residual, sends)
        if step == min(2, len(base_order) - 1):
            tied["late"] = sends
        return gots

    summed = scatter_bits(chains_of(halves, orders, tp_masks, rows_joint), hook, True)[0]
    residual = tied["residual"]

    rows_moe = (residual * gains[1]).astype(bf16)
    expert_total = router.shape[1]
    partial = jnp.concatenate(
        [
            jnp.dot(rows_moe, router, preferred_element_type=f32),
            jnp.sum(residual * residual, axis=-1, keepdims=True),
        ],
        axis=-1,
    )
    high = lax.reduce_precision(partial, 8, 7)
    low = partial - high
    half = LANES // 2
    mine = (row[:, None] - tp_index * tok_dev == jnp.arange(tok_dev)[None, :]).astype(f32)
    ids_rows = jnp.dot(mine, expert_ids.astype(f32), precision=lax.Precision.HIGHEST)
    facts = jnp.concatenate([high, low, ids_rows], axis=-1).astype(bf16)
    facts = jnp.pad(facts, ((0, 0), (0, half - facts.shape[1])))
    outgoing = jnp.concatenate([residual.astype(bf16), facts], axis=-1)
    outgoing = lax.dot_general(
        to_rel, outgoing, (((0,), (0,)), ((), ())), preferred_element_type=f32
    ).astype(bf16)
    out_rows = outgoing[:, :feature_dev].reshape(devices, tok_dev * feature_dev)
    out_facts = outgoing[:, feature_dev:].reshape(rep_count, 1, per_rep * half)
    out_facts = jnp.broadcast_to(out_facts, (rep_count, tp_count, per_rep * half))
    out_facts = out_facts.reshape(devices, per_rep * half)
    outgoing = jnp.concatenate([out_rows, out_facts], axis=-1)
    incoming = lax.all_to_all(outgoing, AXES, split_axis=0, concat_axis=0, tiled=True)
    incoming = after(incoming, tied["late"])
    mamba_out = incoming[:, : tok_dev * feature_dev].reshape(devices, tok_dev, feature_dev)
    mamba_out = mamba_out.transpose(1, 0, 2).reshape(tok_dev, model)
    facts = incoming[:, tok_dev * feature_dev :].astype(f32).sum(axis=0).reshape(per_rep, half)
    ids_all = facts[:, 2 * (expert_total + 1) : 2 * (expert_total + 1) + 2].astype(jnp.int32)
    facts = facts[:, : expert_total + 1] + facts[:, expert_total + 1 : 2 * (expert_total + 1)]
    moe_scale = lax.rsqrt(facts[:, expert_total:] / model + epsilon)
    logits = facts[:, :expert_total] * moe_scale

    choose = (
        ids_all[:, :, None] == jnp.arange(expert_total, dtype=jnp.int32)[None, None, :]
    ).astype(f32)
    picked = jnp.sum(choose * logits[:, None, :], axis=2)
    first_gate = jax.nn.sigmoid(picked[:, 0] - picked[:, 1])
    second_gate = jax.nn.sigmoid(picked[:, 1] - picked[:, 0])
    window_count = expert_proj.shape[1]
    window = jnp.arange(window_count, dtype=jnp.int32)
    names_first = ids_all[:, 0:1] == window[None, :]
    names_second = ids_all[:, 1:2] == window[None, :]
    zero = jnp.zeros((), f32)
    gate_w = jnp.where(names_first, first_gate[:, None], zero) + jnp.where(
        names_second, second_gate[:, None], zero
    )
    gate_w = gate_w.astype(bf16).astype(f32)
    routed = (names_first | names_second).astype(jnp.int32).reshape(tp_count, tok_dev, window_count)
    position = jnp.cumsum(routed, axis=1) - routed
    slot_of = (position[..., None] == jnp.arange(CAPACITY, dtype=jnp.int32)) & (
        routed[..., None] > 0
    )
    gate_up = summed * moe_scale[None, None]
    hidden = gate_w.T[:, :, None] * jax.nn.silu(gate_up[:, 0]) * gate_up[:, 1]
    hidden = hidden.astype(bf16).reshape(window_count, tp_count, tok_dev, -1)
    expert_hidden = jnp.einsum(
        "jtec,ejtf->jecf", slot_of.astype(bf16), hidden, preferred_element_type=f32
    ).astype(bf16)
    expert_hidden = expert_hidden.reshape(tp_count * window_count * CAPACITY, -1)
    return (mamba_out, conv_next, ssm_next, expert_hidden)


def solution(mesh):
    in_specs = (
        P(("rep", "tp"), None),
        P(None, "rep", "tp"),
        P("rep", None, "tp"),
        P(None, ("rep", "tp")),
        P(None, ("rep", "tp")),
        P(None, ("rep", "tp")),
        P(("rep", "tp")),
        P(None, ("rep", "tp")),
        P(("rep", "tp"), None, None),
        P("tp", "rep"),
        P(("rep", "tp"), None),
        P(None, ("rep", "tp")),
        P(("rep", "tp"), None),
        P(("rep", "tp"), None, None, None),
        P(("rep", "tp"), None),
    )
    out_specs = (P(("rep", "tp"), None), P(None, "rep", "tp"), P("rep", None, "tp"), P("rep", "tp"))
    return jax.shard_map(shards, mesh=mesh, in_specs=in_specs, out_specs=out_specs, check_vma=False)
```
